32 devices in a mesh: batch: 4 (over y, x), cols: 8 (over z, core).
Axes of the slice: x: 2, y: 2, z: 4, core: 2. Of those that a mesh axis runs over, the one named last changes fastest.
Arguments:
- grad_query: float32 [4, 2048, 2048], P('batch', None, 'cols'), may hold values from -0.875 to 0.875
- grad_key: float32 [4, 2048, 2048], P('batch', None, 'cols'), may hold values from -0.875 to 0.875
- grad_value: float32 [4, 2048, 2048], P('batch', None, 'cols'), may hold values from -0.875 to 0.875
- grad_mixed: float32 [4, 2048, 2048], P('batch', 'cols'), may hold values from -0.875 to 0.875
- grad_norm: float32 [4, 2048], P('batch'), may hold values from -8 to 8
- grad_bias: float32 [4, 2048], P('batch'), may hold values from -8 to 8
- weight_query: float32 [2048, 2048], P('batch', 'cols'), may hold values from -0.1875 to 0.1875
- weight_key: float32 [2048, 2048], P('batch', 'cols'), may hold values from -0.1875 to 0.1875
- weight_value: float32 [2048, 2048], P('batch', 'cols'), may hold values from -0.1875 to 0.1875
- weight_mixed: float32 [2048, 2048], P('cols', 'batch'), may hold values from -0.1875 to 0.1875
- weight_norm: float32 [2048], P('batch'), may hold values from 0.25 to 1.75
- weight_bias: float32 [2048], P('batch'), may hold values from -3 to 3
Outputs:
- copy_query: bfloat16 [2048, 2048], P(None, 'cols')
- copy_key: bfloat16 [2048, 2048], P(None, 'cols')
- copy_value: bfloat16 [2048, 2048], P(None, 'cols')
- copy_mixed: bfloat16 [2048, 2048], P('cols')
- copy_norm: bfloat16 [2048], replicated
- copy_bias: bfloat16 [2048], replicated
- new_query: float32 [2048, 2048], P('batch', 'cols')
- new_key: float32 [2048, 2048], P('batch', 'cols')
- new_value: float32 [2048, 2048], P('batch', 'cols')
- new_mixed: float32 [2048, 2048], P('cols', 'batch')
- new_norm: float32 [2048], P('batch')
- new_bias: float32 [2048], P('batch')
The draws below stay inside these ranges and needn't reach their ends.
All inputs are finite; a program needn't handle non-finite values.
Results may differ from the reference program's by a relative error of at most 0.0004.
Values may be sent and summed in bfloat16 or wider, within the bound.
No kernel may reach another device: no remote copies, remote signals or barrier semaphores. Data moves between devices by JAX's collectives and lax.ppermute only.
A program may use at most 64 MiB of HBM per device.

```python
import jax
import jax.numpy as jnp
from jax import lax

WIDTH = 2048
ATTN = 2048
REPLICAS = 4


def strengthened(entries, own_key, source, target, shards_of, factor):
    owner, partner = [(jnp.arange(entries.shape[position]) // (entries.shape[position] // shards_of)).reshape([-1 if axis == position else 1 for axis in range(entries.ndim)]) for position in (source, target)]
    chosen = jax.random.permutation(own_key, shards_of)[partner]
    strong = (owner == chosen) | (owner == (partner + shards_of // 2) % shards_of)
    return jnp.where(strong, factor * entries, entries)


def block_scale(key, shape, split, low, largest):
    level, own = 1.0, jax.random.fold_in(key, 6)
    for position, parts in split:
        steps = jnp.exp(jax.random.uniform(jax.random.fold_in(own, position), (parts,), jnp.float32, low / len(split), largest / len(split)))
        level = level * jnp.repeat(steps, shape[position] // parts).reshape([-1 if axis == position else 1 for axis in range(len(shape))])
    return level


def bell_draw(rng, extent, deviation, bound, cuts=(), held_as=jnp.bfloat16):
    values = jax.random.normal(rng, extent, jnp.float32) * deviation
    if len(cuts) > 0:
        values = block_scale(rng, extent, cuts, -0.22, 0.18) * values
    return jnp.clip(values, min=-bound, max=bound).astype(held_as)


def bell_draw_with(key, shape, deviation, most, split, heavy, held_as=jnp.bfloat16):
    entries = deviation * jax.random.normal(key, shape, jnp.float32)
    if split:
        entries = entries * block_scale(key, shape, split, -0.22, 0.18)
    return jnp.clip(strengthened(entries, jax.random.fold_in(key, 3), *heavy), -most, most).astype(held_as)


def setup_inputs(seed: int = 0) -> dict:
    seeds = jax.random.split(jax.random.key(seed), 13)
    grad_query = bell_draw_with(seeds[0], (REPLICAS, WIDTH, ATTN), 0.1, 0.875, ((0, 4), (2, 8)), (0, 1, 4, 2.0), jnp.float32)
    grad_key = bell_draw_with(seeds[1], (REPLICAS, WIDTH, ATTN), 0.1, 0.875, ((0, 4), (2, 8)), (0, 1, 4, 2.0), jnp.float32)
    grad_value = bell_draw_with(seeds[2], (REPLICAS, WIDTH, ATTN), 0.1, 0.875, ((0, 4), (2, 8)), (0, 1, 4, 2.0), jnp.float32)
    grad_mixed = bell_draw_with(seeds[3], (REPLICAS, ATTN, WIDTH), 0.1, 0.875, ((0, 4), (1, 8)), (0, 2, 4, 2.0), jnp.float32)
    grad_norm = bell_draw_with(seeds[4], (REPLICAS, WIDTH), 1.0, 8.0, ((0, 4),), (0, 1, 4, 2.0), jnp.float32)
    grad_bias = bell_draw_with(seeds[5], (REPLICAS, WIDTH), 1.0, 8.0, ((0, 4),), (0, 1, 4, 2.0), jnp.float32)
    weight_query = bell_draw_with(seeds[6], (WIDTH, ATTN), WIDTH ** -0.5, 0.1875, ((0, 4), (1, 8)), (1, 0, 8, 2.0), jnp.float32)
    weight_key = bell_draw_with(seeds[7], (WIDTH, ATTN), WIDTH ** -0.5, 0.1875, ((0, 4), (1, 8)), (1, 0, 8, 2.0), jnp.float32)
    weight_value = bell_draw_with(seeds[8], (WIDTH, ATTN), WIDTH ** -0.5, 0.1875, ((0, 4), (1, 8)), (1, 0, 8, 2.0), jnp.float32)
    weight_mixed = bell_draw_with(seeds[9], (ATTN, WIDTH), ATTN ** -0.5, 0.1875, ((0, 8), (1, 4)), (0, 1, 8, 2.0), jnp.float32)
    weight_norm = jnp.clip(1.0 + 0.15 * jax.random.normal(seeds[10], (WIDTH,), jnp.float32), 0.25, 1.75)
    weight_bias = bell_draw(seeds[11], (WIDTH,), 0.5, 3.0, ((0, 4),), jnp.float32)
    return dict(grad_query=grad_query, grad_key=grad_key, grad_value=grad_value, grad_mixed=grad_mixed, grad_norm=grad_norm, grad_bias=grad_bias, weight_query=weight_query, weight_key=weight_key, weight_value=weight_value, weight_mixed=weight_mixed, weight_norm=weight_norm, weight_bias=weight_bias)


learn_rate = 0.4

def reference(grad_query, grad_key, grad_value, grad_mixed, grad_norm, grad_bias, weight_query, weight_key, weight_value, weight_mixed, weight_norm, weight_bias):
    mean_query = lax.optimization_barrier(jnp.sum(grad_query.astype(jnp.float32), axis=0)) * REPLICAS ** (-0.5)
    mean_key = lax.optimization_barrier(jnp.sum(grad_key.astype(jnp.float32), axis=0)) * REPLICAS ** (-0.5)
    mean_value = lax.optimization_barrier(jnp.sum(grad_value.astype(jnp.float32), axis=0)) * REPLICAS ** (-0.5)
    mean_mixed = lax.optimization_barrier(jnp.sum(grad_mixed.astype(jnp.float32), axis=0)) * REPLICAS ** (-0.5)
    mean_norm = lax.optimization_barrier(jnp.sum(grad_norm.astype(jnp.float32), axis=0)) * REPLICAS ** (-0.5)
    mean_bias = lax.optimization_barrier(jnp.sum(grad_bias.astype(jnp.float32), axis=0)) * REPLICAS ** (-0.5)
    ratio_query = jnp.sqrt(lax.optimization_barrier(jnp.sum(weight_query * weight_query, axis=1, keepdims=True))) * lax.rsqrt(lax.optimization_barrier(jnp.sum(mean_query * mean_query, axis=1, keepdims=True)) + 1e-06)
    mean_query = mean_query * ratio_query
    ratio_key = jnp.sqrt(lax.optimization_barrier(jnp.sum(weight_key * weight_key, axis=1, keepdims=True))) * lax.rsqrt(lax.optimization_barrier(jnp.sum(mean_key * mean_key, axis=1, keepdims=True)) + 1e-06)
    mean_key = mean_key * ratio_key
    ratio_value = jnp.sqrt(lax.optimization_barrier(jnp.sum(weight_value * weight_value, axis=1, keepdims=True))) * lax.rsqrt(lax.optimization_barrier(jnp.sum(mean_value * mean_value, axis=1, keepdims=True)) + 1e-06)
    mean_value = mean_value * ratio_value
    ratio_mixed = jnp.sqrt(lax.optimization_barrier(jnp.sum(weight_mixed * weight_mixed, axis=0, keepdims=True))) * lax.rsqrt(lax.optimization_barrier(jnp.sum(mean_mixed * mean_mixed, axis=0, keepdims=True)) + 1e-06)
    mean_mixed = mean_mixed * ratio_mixed
    new_query = weight_query - learn_rate * mean_query
    new_key = weight_key - learn_rate * mean_key
    new_value = weight_value - learn_rate * mean_value
    new_mixed = weight_mixed - learn_rate * mean_mixed
    new_norm = weight_norm - learn_rate * mean_norm
    new_bias = weight_bias - learn_rate * mean_bias
    copy_query = new_query.astype(jnp.bfloat16)
    copy_key = new_key.astype(jnp.bfloat16)
    copy_value = new_value.astype(jnp.bfloat16)
    copy_mixed = new_mixed.astype(jnp.bfloat16)
    copy_norm = new_norm.astype(jnp.bfloat16)
    copy_bias = new_bias.astype(jnp.bfloat16)
    return (copy_query, copy_key, copy_value, copy_mixed, copy_norm, copy_bias, new_query, new_key, new_value, new_mixed, new_norm, new_bias)
```

```python
import functools

import jax
import jax.numpy as jnp
from jax import lax
from jax.experimental import pallas as pl
from jax.experimental.pallas import tpu as pltpu
from jax.sharding import PartitionSpec as P

learn_rate = 0.4


def factors(n):
    nx = max(f for f in range(1, n + 1) if n % f == 0 and f * f <= n)
    return n // nx, nx


class Grid:
    def __init__(self):
        self.n = lax.axis_size("batch")
        self.ny, self.nx = factors(self.n)
        index = lax.axis_index("batch")
        self.y, self.x = index // self.nx, index % self.nx

    def shift_x(self, value, k):
        ny, nx = self.ny, self.nx
        pairs = [(y * nx + x, y * nx + (x + k) % nx) for y in range(ny) for x in range(nx)]
        return lax.ppermute(value, "batch", pairs)

    def shift_y(self, value, k):
        ny, nx = self.ny, self.nx
        pairs = [(y * nx + x, (y + k) % ny * nx + x) for y in range(ny) for x in range(nx)]
        return lax.ppermute(value, "batch", pairs)


def sum_cols(value):
    m = lax.axis_size("cols")
    if m & (m - 1):
        return lax.psum(value, "cols")
    step = 1
    while step < m:
        value = value + lax.ppermute(value, "cols", [(i, i ^ step) for i in range(m)])
        step *= 2
    return value


def row_piece(grid, g, y, x, half):
    rows = g.shape[0] // grid.n
    start = (y * grid.nx + x) * rows + half * (rows // 2)
    return lax.dynamic_slice(g, (start, 0), (rows // 2, g.shape[1]))


def column_piece(grid, g, y, x, half):
    columns, rows = g.shape[1] // grid.n, g.shape[0] // 2
    return lax.dynamic_slice(g, (half * rows, (y * grid.nx + x) * columns), (rows, columns))


def scatter_first(grid, g, piece):
    ny, nx, y, x = grid.ny, grid.nx, grid.y, grid.x
    from_x = [
        grid.shift_x(jnp.stack([piece(grid, g, v, (x + k) % nx, 0) for v in range(ny)]), k)
        for k in range(1, nx)
    ]
    from_y = [
        grid.shift_y(jnp.stack([piece(grid, g, (y + k) % ny, u, 1) for u in range(nx)]), k)
        for k in range(1, ny)
    ]
    return from_x, from_y


def scatter_second(grid, g, piece, first):
    ny, nx, y, x = grid.ny, grid.nx, grid.y, grid.x
    from_x, from_y = first

    def partial_0(v):
        return sum((lax.dynamic_index_in_dim(r, v, 0, False) for r in from_x), piece(grid, g, v, x, 0))

    def partial_1(u):
        return sum((lax.dynamic_index_in_dim(r, u, 0, False) for r in from_y), piece(grid, g, y, u, 1))

    got_0 = [grid.shift_y(partial_0((y + k) % ny), k) for k in range(1, ny)]
    got_1 = [grid.shift_x(partial_1((x + k) % nx), k) for k in range(1, nx)]
    return sum(got_0, partial_0(y)), sum(got_1, partial_1(x))


def gather_first(grid, share):
    ny, nx = grid.ny, grid.nx
    from_x = [grid.shift_x(share, k) for k in range(1, nx)]
    from_y = [grid.shift_y(share, k) for k in range(1, ny)]
    return from_x, from_y


def gather_second(grid, share, first, axis):
    ny, nx = grid.ny, grid.nx
    from_x, from_y = first
    half = share.shape[axis] // 2
    low = [[grid.shift_y(lax.slice_in_dim(r, 0, half, axis=axis), k) for r in from_x] for k in range(1, ny)]
    high = [[grid.shift_x(lax.slice_in_dim(r, half, 2 * half, axis=axis), k) for r in from_y] for k in range(1, nx)]
    parts = [((0, 0), 0, share)]
    parts += [((0, k), 0, r) for k, r in enumerate(from_x, 1)]
    parts += [((k, 0), 0, r) for k, r in enumerate(from_y, 1)]
    for a in range(1, ny):
        for b in range(1, nx):
            parts.append(((a, b), 0, low[a - 1][b - 1]))
            parts.append(((a, b), half, high[b - 1][a - 1]))
    return parts


def assemble_kernel(places, rows, axis, nx, index_ref, *refs):
    out = refs[-1]
    for slot, ((offset), ref) in enumerate(zip(places, refs[:-1])):
        block = index_ref[slot]
        if axis == 0:
            start = pl.multiple_of(block * rows + offset, 8)
            out[pl.ds(start, ref.shape[0]), :] = ref[...]
        else:
            start = pl.multiple_of(block * rows, 128)
            out[pl.ds(offset, ref.shape[0]), pl.ds(start, ref.shape[1])] = ref[...]


def assemble(grid, parts, share_shape, axis):
    ny, nx = grid.ny, grid.nx
    index = jnp.stack(
        [(grid.y - a + ny) % ny * nx + (grid.x - b + nx) % nx for (a, b), _, _ in parts]
    ).astype(jnp.int32)
    shape = list(share_shape)
    shape[axis] *= grid.n
    return pl.pallas_call(
        functools.partial(assemble_kernel, [p[1] for p in parts], share_shape[axis], axis, nx),
        out_shape=jax.ShapeDtypeStruct(tuple(shape), jnp.bfloat16),
        in_specs=[pl.BlockSpec(memory_space=pltpu.SMEM)]
        + [pl.BlockSpec(memory_space=pltpu.VMEM)] * len(parts),
        out_specs=pl.BlockSpec(memory_space=pltpu.VMEM),
        name="assemble",
    )(index, *[p[2] for p in parts])


def per_device(
    grad_query,
    grad_key,
    grad_value,
    grad_mixed,
    grad_norm,
    grad_bias,
    weight_query,
    weight_key,
    weight_value,
    weight_mixed,
    weight_norm,
    weight_bias,
):
    grid = Grid()
    rate = grid.n ** (-0.5)
    grads = (grad_query[0], grad_key[0], grad_value[0], grad_mixed[0])
    weights = (weight_query, weight_key, weight_value, weight_mixed)
    pieces = (row_piece, row_piece, row_piece, column_piece)
    sums_over = (1, 1, 1, 0)

    first = [scatter_first(grid, g, p) for g, p in zip(grads, pieces)]

    vectors = jnp.stack([grad_norm[0], grad_bias[0]])
    length = vectors.shape[1] // grid.n
    me = lax.axis_index("batch")
    mine = lax.dynamic_slice(vectors, (0, me * length), (2, length))
    for k in range(1, grid.n):
        to = (me + k) % grid.n
        sent = lax.dynamic_slice(vectors, (0, to * length), (2, length))
        mine = mine + lax.ppermute(sent, "batch", [(i, (i + k) % grid.n) for i in range(grid.n)])
    new_vectors = jnp.stack([weight_norm, weight_bias]) - learn_rate * (mine * rate)
    copies = new_vectors.astype(jnp.bfloat16)
    zeros = jnp.zeros((2, vectors.shape[1]), jnp.bfloat16)
    copy_vectors = lax.dynamic_update_slice(zeros, copies, (0, me * length))
    for k in range(1, grid.n):
        got = lax.ppermute(copies, "batch", [(i, (i + k) % grid.n) for i in range(grid.n)])
        copy_vectors = lax.dynamic_update_slice(copy_vectors, got, (0, (me - k + grid.n) % grid.n * length))

    own = sum_cols(jnp.stack([jnp.sum(w * w, axis=a) for w, a in zip(weights, sums_over)]))

    totals, squares = [], []
    for g, p, f, a in zip(grads, pieces, first, sums_over):
        total = jnp.concatenate(scatter_second(grid, g, p, f), axis=0) * rate
        totals.append(total)
        squares.append(jnp.sum(total * total, axis=a))
    slopes = []
    for start in range(0, 4, 2):
        both = sum_cols(jnp.stack(squares[start : start + 2]))
        slopes += [both[0], both[1]]
    news, shares = [], []
    for i, (w, t, s, a) in enumerate(zip(weights, totals, slopes, sums_over)):
        ratio = jnp.sqrt(own[i]) * lax.rsqrt(s + 1e-06)
        new = w - learn_rate * (t * jnp.expand_dims(ratio, a))
        news.append(new)
        shares.append(new.astype(jnp.bfloat16))
    gathered = [gather_first(grid, s) for s in shares]
    outs = []
    for i, (s, f) in enumerate(zip(shares, gathered)):
        parts = gather_second(grid, s, f, 0)
        outs.append(assemble(grid, parts, s.shape, 0 if i < 3 else 1))
    return (
        *outs,
        copy_vectors[0],
        copy_vectors[1],
        *news,
        new_vectors[0],
        new_vectors[1],
    )


def solution(mesh):
    in_specs = (
        P("batch", None, "cols"),
        P("batch", None, "cols"),
        P("batch", None, "cols"),
        P("batch", "cols", None),
        P("batch", None),
        P("batch", None),
        P("batch", "cols"),
        P("batch", "cols"),
        P("batch", "cols"),
        P("cols", "batch"),
        P("batch"),
        P("batch"),
    )
    out_specs = (
        P(None, "cols"),
        P(None, "cols"),
        P(None, "cols"),
        P("cols", None),
        P(),
        P(),
        P("batch", "cols"),
        P("batch", "cols"),
        P("batch", "cols"),
        P("cols", "batch"),
        P("batch"),
        P("batch"),
    )
    return jax.shard_map(
        per_device, mesh=mesh, in_specs=in_specs, out_specs=out_specs, check_vma=False
    )
```
